32 devices in a mesh: row: 2 (over y), col: 4 (over x, core), band: 4 (over z).
Axes of the slice: x: 2, y: 2, z: 4, core: 2. Of those that a mesh axis runs over, the one named last changes fastest.
Arguments:
- noisy: float32 [224, 32, 4096], P('band', 'row', 'col'), may hold values from -4 to 4
- weight_map: float32 [32, 4096], P('row', 'col'), may hold values from 1.5 to 12
Outputs:
- denoised: float32 [224, 32, 4096], P('band', 'row', 'col')
The draws below stay inside these ranges and needn't reach their ends.
All inputs are finite; a program needn't handle non-finite values.
Results may differ from the reference program's by a relative error of at most 0.0001.
Values sent between devices are 32-bit elements; how exact they have to be, the bound alone decides.
A program may use at most 64 MiB of HBM per device.

```python
import math
import jax
import jax.numpy as jnp
from jax import lax

BANDS = 224
COLS = 4096
ITERS = 4
ROWS = 32


def draw_noisy(key, part):
    key_center, key_texture = jax.random.split(jax.random.fold_in(key, 17))
    center = jax.random.randint(key_center, (), 0, BANDS).astype(jnp.float32)
    spread = BANDS / 16.0
    texture = jnp.clip(jax.random.normal(key_texture, (BANDS, ROWS, COLS), jnp.float32), -4.0, 4.0)
    offset = (jnp.arange(BANDS, dtype=jnp.float32) - center) / spread
    profile = 0.1 + 0.9 * jnp.exp(-0.5 * offset * offset)
    return (profile[:, None, None] * texture).astype(jnp.float32)


def shard_levels(key, extent, cuts, low, top_value):
    level = 1.0
    for dim, shards_of in cuts:
        steps = jax.random.uniform(jax.random.fold_in(jax.random.fold_in(key, 6), dim), (shards_of,), jnp.float32, low / len(cuts), top_value / len(cuts))
        level = level * jnp.repeat(jnp.exp(steps), extent[dim] // shards_of).reshape((-1,) + (1,) * (len(extent) - 1 - dim))
    return level


def setup_inputs(seed: int = 0) -> dict:
    key_of = jax.random.split(jax.random.key(seed), 3)
    noisy = draw_noisy(jax.random.fold_in(key_of[2], 71), 0)
    weight_map = jnp.clip(jnp.exp(math.log(12.0) - 2.0794415 * jax.random.uniform(key_of[1], (ROWS, COLS), jnp.float32) ** shard_levels(key_of[1], (ROWS, COLS), ((0, 2), (1, 4)), -0.2, 0.2)), 1.5, 12.0)
    return {"noisy": noisy, "weight_map": weight_map}


dual_step = 0.35
primal_step = 0.35

def forward_diff(field):
    zeros_row = jnp.zeros_like(field[:, :1, :])
    zeros_col = jnp.zeros_like(field[:, :, :1])
    grad_x = jnp.concatenate([field[:, 1:, :] - field[:, :-1, :], zeros_row], axis=1)
    grad_y = jnp.concatenate([field[:, :, 1:] - field[:, :, :-1], zeros_col], axis=2)
    return (grad_x, grad_y)

def divergence(first, second):
    masked_a = first.at[:, -1, :].set(0.0)
    masked_b = second.at[:, :, -1].set(0.0)
    above = jnp.concatenate([jnp.zeros_like(masked_a[:, :1, :]), masked_a[:, :-1, :]], axis=1)
    left = jnp.concatenate([jnp.zeros_like(masked_b[:, :, :1]), masked_b[:, :, :-1]], axis=2)
    return masked_a - above + (masked_b - left)

def reference(noisy, weight_map):
    groups = math.gcd(BANDS, 8)
    rows = noisy.shape[1]
    cols = noisy.shape[2]
    source = noisy.reshape(groups, BANDS // groups, rows, cols)
    primal = source
    extra = source
    dual_x = jnp.zeros_like(source)
    dual_y = jnp.zeros_like(source)
    for step in range(ITERS):

        def dual_part(items):
            ubar, first, second = items
            grad_x, grad_y = forward_diff(ubar)
            qx = first + dual_step * grad_x
            qy = second + dual_step * grad_y
            return (qx, qy, lax.optimization_barrier(jnp.sum(qx * qx + qy * qy, axis=0)))
        qxs, qys, partial_value = lax.map(dual_part, (extra, dual_x, dual_y))
        squares = lax.optimization_barrier(jnp.sum(partial_value, axis=0))
        scale = weight_map / jnp.maximum(weight_map, jnp.sqrt(1.0 + squares))

        def primal_part(items):
            qx, qy, older, given = items
            first = scale * qx
            second = scale * qy
            newer = (older + primal_step * divergence(first, second) + primal_step * given) / (1.0 + primal_step)
            return (first, second, newer, 2.0 * newer - older)
        dual_x, dual_y, primal, extra = lax.map(primal_part, (qxs, qys, primal, source))
    return primal.reshape(BANDS, rows, cols)
```

```python
import functools

import jax
import jax.numpy as jnp
from jax import lax
from jax.experimental import pallas as pl
from jax.experimental.pallas import tpu as pltpu
from jax.sharding import PartitionSpec as P

ITERS = 4
dual_step = 0.35
primal_step = 0.35
KEEP = 1.0 / (1.0 + primal_step)
GAIN = primal_step / (1.0 + primal_step)
STEP = GAIN * dual_step
LANES = 128
MESH = pl.DeviceIdType.MESH


def kernel(n_row, n_col, n_band, x_ref, w_ref, out_ref,
           N, U, W, QX, QY, HU, HD, E, ER, EL, WT, SC, CY, S, SE, R, RE,
           in_sem, out_sem, ys, yr, xs, xr, zs, zr):
    rows, bands, cols = x_ref.shape
    wide = cols + LANES
    groups = bands // 8
    last = rows - 1
    ri = lax.axis_index("row")
    ci = lax.axis_index("col")
    bi = lax.axis_index("band")
    has_up = ri > 0
    has_down = ri < n_row - 1
    has_left = ci > 0
    has_right = ci < n_col - 1

    fetch = pltpu.make_async_copy(x_ref, N.at[:, 0:bands, 0:cols], in_sem)
    fetch.start()

    barrier = pltpu.get_barrier_semaphore()
    for cond, axis, target in ((has_up, "row", ri - 1), (has_down, "row", ri + 1),
                               (has_left, "col", ci - 1), (has_right, "col", ci + 1)):
        @pl.when(cond)
        def _():
            pl.semaphore_signal(barrier, inc=1, device_id={axis: target}, device_id_type=MESH)
    for d in range(1, n_band):
        pl.semaphore_signal(barrier, inc=1, device_id={"band": lax.rem(bi + d, n_band)}, device_id_type=MESH)
    count = (n_band - 1 + has_up.astype(jnp.int32) + has_down.astype(jnp.int32)
             + has_left.astype(jnp.int32) + has_right.astype(jnp.int32))

    def up_copy(i, src, dst):
        return pltpu.make_async_remote_copy(
            src_ref=src, dst_ref=dst, send_sem=ys.at[0, i], recv_sem=yr.at[0, i],
            device_id={"row": ri - 1}, device_id_type=MESH)

    def down_copy(i, src, dst):
        return pltpu.make_async_remote_copy(
            src_ref=src, dst_ref=dst, send_sem=ys.at[1, i], recv_sem=yr.at[1, i],
            device_id={"row": ri + 1}, device_id_type=MESH)

    def y_pair(k, part):
        if k == 0:
            span = pl.ds(0, cols) if part == 0 else pl.ds(cols, LANES)
            i = 0 if part == 0 else ITERS
            return (up_copy(i, N.at[0, :, span], HU.at[0, :, span]),
                    down_copy(i, N.at[last, :, span], HD.at[0, :, span]))
        span = pl.ds(0, bands)
        return (up_copy(k, W.at[0], HU.at[k, span]), down_copy(k, W.at[last], HD.at[k, span]))

    def y_start(k, part=0):
        up, down = y_pair(k, part)

        @pl.when(has_up)
        def _():
            up.start()

        @pl.when(has_down)
        def _():
            down.start()

    def y_recv(k, part=0):
        up, down = y_pair(k, part)

        @pl.when(has_down)
        def _():
            up.wait_recv()

        @pl.when(has_up)
        def _():
            down.wait_recv()

    def y_sent(k, part=0):
        up, down = y_pair(k, part)

        @pl.when(has_up)
        def _():
            up.wait_send()

        @pl.when(has_down)
        def _():
            down.wait_send()

    def z_copy(k, d, part):
        if part < 2:
            half = pl.ds(part * 8, 8)
            src, dst = S.at[k, half], R.at[k, d - 1, half]
        else:
            src, dst = SE.at[k], RE.at[k, d - 1]
        return pltpu.make_async_remote_copy(
            src_ref=src, dst_ref=dst, send_sem=zs.at[k, d - 1, part], recv_sem=zr.at[k, d - 1, part],
            device_id={"band": lax.rem(bi + d, n_band)}, device_id_type=MESH)

    def z_start(k, part):
        for d in range(1, n_band):
            z_copy(k, d, part).start()

    def total(k, part):
        for d in range(1, n_band):
            z_copy(k, d, part).wait_recv()
        if part < 2:
            half = pl.ds(part * 8, 8)
            acc = S[k, half]
            for d in range(1, n_band):
                acc = acc + R[k, d - 1, half]
            return acc
        acc = SE[k]
        for d in range(1, n_band):
            acc = acc + RE[k, d - 1]
        return acc

    def scale_of(weight, squares):
        return weight / jnp.maximum(weight, jnp.sqrt(1.0 + squares * (1.0 / (GAIN * GAIN))))

    def sync(k):
        for part in range(2):
            half = pl.ds(part * 8, 8)
            SC[half] = scale_of(WT[half], total(k, part))
        edge = total(k, 2)
        SC[pl.ds(last, 1)] = scale_of(WT[pl.ds(last, 1)], edge[0:1])
        SC[pl.ds(rows, 1)] = scale_of(WT[pl.ds(rows, 1)], edge[1:2])

    def left_of(v):
        return pltpu.roll(v, 1, 1)

    def right_of(v):
        return pltpu.roll(v, wide - 1, 1)

    pl.semaphore_wait(barrier, count)

    lane = lax.broadcasted_iota(jnp.int32, (1, wide), 1)
    column = ci * cols + jnp.where(lane < cols + LANES // 2, lane, lane - wide)
    CY[...] = jnp.where((column >= 0) & (column < n_col * cols - 1), STEP, 0.0)

    def put_weight(r, _):
        N[r, pl.ds(bands, 8), 0:cols] = jnp.broadcast_to(w_ref[pl.ds(r, 1), :], (8, cols))
        return 0
    lax.fori_loop(0, rows, put_weight, 0)
    S[:, pl.ds(8, 8), :] = jnp.zeros((ITERS, 8, wide), jnp.float32)

    @pl.when(jnp.logical_not(has_down))
    def _():
        HU[...] = jnp.zeros_like(HU)

    @pl.when(jnp.logical_not(has_up))
    def _():
        HD[...] = jnp.zeros_like(HD)

    @pl.when(jnp.logical_not(has_right))
    def _():
        ER[...] = jnp.zeros_like(ER)

    @pl.when(jnp.logical_not(has_left))
    def _():
        EL[...] = jnp.zeros_like(EL)

    fetch.wait()
    y_start(0, 0)

    pitch = 2 * ITERS
    spot = lax.broadcasted_iota(jnp.int32, (8, LANES), 1)

    def pack(g, _):
        span = pl.ds(pl.multiple_of(g * 8, 8), 8)
        acc = jnp.zeros((8, LANES), jnp.float32)
        for r in range(rows):
            at = r * pitch
            head = pltpu.roll(N[r, span, 0:LANES], at % LANES, 1)
            tail = pltpu.roll(N[r, span, cols - LANES:cols], (at + pitch) % LANES, 1)
            acc = jnp.where((spot >= at) & (spot < at + ITERS), head, acc)
            acc = jnp.where((spot >= at + ITERS) & (spot < at + pitch), tail, acc)
        E[span] = acc
        return 0
    lax.fori_loop(0, groups + 1, pack, 0)

    to_left = pltpu.make_async_remote_copy(
        src_ref=E, dst_ref=ER, send_sem=xs.at[0], recv_sem=xr.at[0],
        device_id={"col": ci - 1}, device_id_type=MESH)
    to_right = pltpu.make_async_remote_copy(
        src_ref=E, dst_ref=EL, send_sem=xs.at[1], recv_sem=xr.at[1],
        device_id={"col": ci + 1}, device_id_type=MESH)

    @pl.when(has_left)
    def _():
        to_left.start()

    @pl.when(has_right)
    def _():
        to_right.start()

    @pl.when(has_right)
    def _():
        to_left.wait_recv()

    @pl.when(has_left)
    def _():
        to_right.wait_recv()

    def unpack(g, _):
        span = pl.ds(pl.multiple_of(g * 8, 8), 8)
        from_right, from_left = ER[span], EL[span]
        for r in range(rows):
            at = r * pitch
            head = pltpu.roll(from_right, (LANES - at) % LANES, 1)
            tail = pltpu.roll(from_left, (LANES - at - pitch) % LANES, 1)
            N[r, span, cols:wide] = jnp.where(spot < LANES // 2, head, tail)
        return 0
    lax.fori_loop(0, groups + 1, unpack, 0)
    y_start(0, 1)

    def put_wt(r, _):
        WT[pl.ds(r, 1)] = N[r, pl.ds(bands, 1), :]
        return 0
    lax.fori_loop(0, rows, put_wt, 0)

    def span_of(g):
        return pl.ds(g * 8, 8)

    def group_sum(acc):
        return jnp.sum(acc, axis=0, keepdims=True)

    def dual_row(r, own, nxt, cx, first):
        acc = jnp.zeros((8, wide), jnp.float32)
        cy = CY[...]
        sc = None if first else SC[pl.ds(r, 1)]
        for g in range(groups):
            wu, w = own(g), nxt(g)
            qx = cx * (w - wu)
            qy = cy * (right_of(wu) - wu)
            if not first:
                qx = sc * QX[r, span_of(g)] + qx
                qy = sc * QY[r, span_of(g)] + qy
            QX[r, span_of(g)] = qx
            QY[r, span_of(g)] = qy
            acc = acc + (qx * qx + qy * qy)
        return group_sum(acc)

    cx_last = jnp.where(has_down, STEP, 0.0)
    cx_above = jnp.where(has_up, STEP, 0.0)

    def edges(k, field):
        y_recv(k, 0)
        if k == 0:
            y_recv(0, 1)
            WT[pl.ds(rows, 1)] = HD[0, pl.ds(bands, 1), :]
        SE[k, pl.ds(0, 1)] = dual_row(last, lambda g: field[last, span_of(g)],
                                      lambda g: HU[k, span_of(g)], cx_last, k == 0)
        SE[k, pl.ds(1, 1)] = dual_row(rows, lambda g: HD[k, span_of(g)],
                                      lambda g: field[0, span_of(g)], cx_above, k == 0)
        z_start(k, 2)

    def primal_group(r, above, g, first):
        sc, su = SC[pl.ds(r, 1)], SC[pl.ds(above, 1)]
        pu = su * QX[above, span_of(g)]
        px = sc * QX[r, span_of(g)]
        py = sc * QY[r, span_of(g)]
        div = (px - pu) + (py - left_of(py))
        given = N[r, span_of(g)]
        if first:
            u = given
            new = given + div
        else:
            u = U[r, span_of(g)]
            new = KEEP * u + (GAIN * given + div)
        U[r, span_of(g)] = new
        return pu, new, u

    def primal_row(r, above, first):
        for g in range(groups):
            _, new, u = primal_group(r, above, g, first)
            W[r, span_of(g)] = 2.0 * new - u

    def start_row(r, _):
        S[0, pl.ds(r, 1)] = dual_row(r, lambda g: N[r, span_of(g)], lambda g: N[r + 1, span_of(g)], STEP, True)
        return 0
    lax.fori_loop(0, 8, start_row, 0)
    z_start(0, 0)
    lax.fori_loop(8, last, start_row, 0)
    z_start(0, 1)
    edges(0, N)
    sync(0)

    for k in range(1, ITERS):
        first = k == 1
        if k > 1:
            y_sent(k - 1)
        primal_row(0, rows, first)
        primal_row(last, last - 1, first)
        y_start(k)

        def both(r, _, first=first, k=k):
            acc = jnp.zeros((8, wide), jnp.float32)
            cy = CY[...]
            su = SC[pl.ds(r - 1, 1)]
            for g in range(groups):
                pu, new, u = primal_group(r, r - 1, g, first)
                w = 2.0 * new - u
                W[r, span_of(g)] = w
                wu = W[r - 1, span_of(g)]
                qx = pu + STEP * (w - wu)
                qy = su * QY[r - 1, span_of(g)] + cy * (right_of(wu) - wu)
                QX[r - 1, span_of(g)] = qx
                QY[r - 1, span_of(g)] = qy
                acc = acc + (qx * qx + qy * qy)
            S[k, pl.ds(r - 1, 1)] = group_sum(acc)
            return 0
        lax.fori_loop(1, 9, both, 0)
        z_start(k, 0)
        lax.fori_loop(9, last, both, 0)
        S[k, pl.ds(last - 1, 1)] = dual_row(last - 1, lambda g: W[last - 1, span_of(g)],
                                            lambda g: W[last, span_of(g)], STEP, False)
        z_start(k, 1)
        edges(k, W)
        sync(k)

    def finish(r, above):
        for g in range(groups):
            primal_group(r, above, g, False)
        pltpu.make_async_copy(U.at[r, :, 0:cols], out_ref.at[r], out_sem.at[r]).start()

    finish(0, rows)

    def finish_row(r, _):
        finish(r, r - 1)
        return 0
    lax.fori_loop(1, rows, finish_row, 0)

    y_sent(0, 0)
    y_sent(0, 1)
    y_sent(ITERS - 1)

    @pl.when(has_left)
    def _():
        to_left.wait_send()

    @pl.when(has_right)
    def _():
        to_right.wait_send()
    for k in range(ITERS):
        for d in range(1, n_band):
            for part in range(3):
                z_copy(k, d, part).wait_send()

    def drain(r, _):
        pltpu.make_async_copy(U.at[r, :, 0:cols], out_ref.at[r], out_sem.at[r]).wait()
        return 0
    lax.fori_loop(0, rows, drain, 0)


def local(n_row, n_col, n_band, noisy, weight_map):
    bands, rows, cols = noisy.shape
    padded = -(-bands // 8) * 8
    x = jnp.transpose(noisy, (1, 0, 2))
    if padded != bands:
        x = jnp.pad(x, ((0, 0), (0, padded - bands), (0, 0)))
    wide = cols + LANES
    f32 = jnp.float32
    peers = n_band - 1
    dma = pltpu.SemaphoreType.DMA
    out = pl.pallas_call(
        functools.partial(kernel, n_row, n_col, n_band),
        out_shape=jax.ShapeDtypeStruct((rows, padded, cols), f32),
        in_specs=[pl.BlockSpec(memory_space=pl.ANY), pl.BlockSpec(memory_space=pltpu.VMEM)],
        out_specs=pl.BlockSpec(memory_space=pl.ANY),
        scratch_shapes=[
            pltpu.VMEM((rows, padded + 8, wide), f32),
            pltpu.VMEM((rows, padded, wide), f32),
            pltpu.VMEM((rows, padded, wide), f32),
            pltpu.VMEM((rows + 1, padded, wide), f32),
            pltpu.VMEM((rows + 1, padded, wide), f32),
            pltpu.VMEM((ITERS, padded + 8, wide), f32),
            pltpu.VMEM((ITERS, padded + 8, wide), f32),
            pltpu.VMEM((padded + 8, LANES), f32),
            pltpu.VMEM((padded + 8, LANES), f32),
            pltpu.VMEM((padded + 8, LANES), f32),
            pltpu.VMEM((rows + 8, wide), f32),
            pltpu.VMEM((rows + 8, wide), f32),
            pltpu.VMEM((1, wide), f32),
            pltpu.VMEM((ITERS, rows, wide), f32),
            pltpu.VMEM((ITERS, 2, wide), f32),
            pltpu.VMEM((ITERS, peers, rows, wide), f32),
            pltpu.VMEM((ITERS, peers, 2, wide), f32),
            dma, dma((rows,)),
            dma((2, ITERS + 1)), dma((2, ITERS + 1)),
            dma((2,)), dma((2,)),
            dma((ITERS, peers, 3)), dma((ITERS, peers, 3)),
        ],
        compiler_params=pltpu.CompilerParams(
            collective_id=0, has_side_effects=True, vmem_limit_bytes=48 * 1024 * 1024),
    )(x, weight_map)
    return jnp.transpose(out[:, :bands], (1, 0, 2))


def solution(mesh):
    placed = (P("band", "row", "col"), P("row", "col"))
    sizes = dict(mesh.shape)
    body = functools.partial(local, sizes["row"], sizes["col"], sizes["band"])
    return jax.shard_map(
        body, mesh=mesh, in_specs=placed, out_specs=P("band", "row", "col"), check_vma=False
    )
```

```python
import functools

import jax
import jax.numpy as jnp
from jax import lax
from jax.experimental import pallas as pl
from jax.experimental.pallas import tpu as pltpu
from jax.sharding import PartitionSpec as P

ITERS = 4
dual_step = 0.35
primal_step = 0.35
KEEP = 1.0 / (1.0 + primal_step)
GAIN = primal_step / (1.0 + primal_step)
STEP = GAIN * dual_step
LANES = 128
MESH = pl.DeviceIdType.MESH


def kernel(n_row, n_col, n_band, x_ref, w_ref, out_ref,
           N, U, W, QX, QY, HU, HD, E, ER, EL, WT, SC, CY, S, SE, R, RE,
           LA, LB, FA, FB, MA, MB,
           in_sem, out_sem, ys, yr, xs, xr, zs, zr):
    rows, bands, cols = x_ref.shape
    wide = cols + LANES
    groups = bands // 8
    last = rows - 1
    ri = lax.axis_index("row")
    ci = lax.axis_index("col")
    bi = lax.axis_index("band")
    has_up = ri > 0
    has_down = ri < n_row - 1
    has_left = ci > 0
    has_right = ci < n_col - 1

    fetch = pltpu.make_async_copy(x_ref, N.at[:, 0:bands, 0:cols], in_sem)
    fetch.start()

    barrier = pltpu.get_barrier_semaphore()
    for cond, axis, target in ((has_up, "row", ri - 1), (has_down, "row", ri + 1),
                               (has_left, "col", ci - 1), (has_right, "col", ci + 1)):
        @pl.when(cond)
        def _():
            pl.semaphore_signal(barrier, inc=1, device_id={axis: target}, device_id_type=MESH)
    for d in range(1, n_band):
        pl.semaphore_signal(barrier, inc=1, device_id={"band": lax.rem(bi + d, n_band)}, device_id_type=MESH)
    count = (n_band - 1 + has_up.astype(jnp.int32) + has_down.astype(jnp.int32)
             + has_left.astype(jnp.int32) + has_right.astype(jnp.int32))

    def up_copy(i, src, dst):
        return pltpu.make_async_remote_copy(
            src_ref=src, dst_ref=dst, send_sem=ys.at[0, i], recv_sem=yr.at[0, i],
            device_id={"row": ri - 1}, device_id_type=MESH)

    def down_copy(i, src, dst):
        return pltpu.make_async_remote_copy(
            src_ref=src, dst_ref=dst, send_sem=ys.at[1, i], recv_sem=yr.at[1, i],
            device_id={"row": ri + 1}, device_id_type=MESH)

    def y_pair(k, part):
        if k == 0:
            span = pl.ds(0, cols) if part == 0 else pl.ds(cols, LANES)
            i = 0 if part == 0 else ITERS
            return (up_copy(i, N.at[0, :, span], HU.at[0, :, span]),
                    down_copy(i, N.at[last, :, span], HD.at[0, :, span]))
        span = pl.ds(0, bands)
        return (up_copy(k, W.at[0], HU.at[k, span]), down_copy(k, W.at[last], HD.at[k, span]))

    def y_start(k, part=0):
        up, down = y_pair(k, part)

        @pl.when(has_up)
        def _():
            up.start()

        @pl.when(has_down)
        def _():
            down.start()

    def y_recv(k, part=0):
        up, down = y_pair(k, part)

        @pl.when(has_down)
        def _():
            up.wait_recv()

        @pl.when(has_up)
        def _():
            down.wait_recv()

    def y_sent(k, part=0):
        up, down = y_pair(k, part)

        @pl.when(has_up)
        def _():
            up.wait_send()

        @pl.when(has_down)
        def _():
            down.wait_send()

    def z_copy(k, d, part):
        if part < 2:
            half = pl.ds(part * 8, 8)
            src, dst = S.at[k, half], R.at[k, d - 1, half]
        else:
            src, dst = SE.at[k], RE.at[k, d - 1]
        return pltpu.make_async_remote_copy(
            src_ref=src, dst_ref=dst, send_sem=zs.at[k, d - 1, part], recv_sem=zr.at[k, d - 1, part],
            device_id={"band": lax.rem(bi + d, n_band)}, device_id_type=MESH)

    def z_start(k, part):
        for d in range(1, n_band):
            z_copy(k, d, part).start()

    def total(k, part):
        for d in range(1, n_band):
            z_copy(k, d, part).wait_recv()
        if part < 2:
            half = pl.ds(part * 8, 8)
            acc = S[k, half]
            for d in range(1, n_band):
                acc = acc + R[k, d - 1, half]
            return acc
        acc = SE[k]
        for d in range(1, n_band):
            acc = acc + RE[k, d - 1]
        return acc

    def scale_of(weight, squares):
        return weight / jnp.maximum(weight, jnp.sqrt(1.0 + squares * (1.0 / (GAIN * GAIN))))

    def put_scale(r, v):
        SC[r] = jnp.broadcast_to(v, (8, wide))

    def sync(k):
        for part in range(2):
            half = pl.ds(part * 8, 8)
            values = scale_of(WT[half], total(k, part))
            for i in range(8):
                if part * 8 + i < last:
                    put_scale(part * 8 + i, values[i:i + 1])
        edge = total(k, 2)
        put_scale(last, scale_of(WT[pl.ds(last, 1)], edge[0:1]))
        put_scale(rows, scale_of(WT[pl.ds(rows, 1)], edge[1:2]))

    tiles = wide // LANES
    pitch_m = LA.shape[0] // tiles

    def tile(j):
        return pl.ds((j % tiles) * LANES, LANES)

    def part_of(F, j):
        at = (j % tiles) * pitch_m
        return F.at[pl.ds(at, bands), 0:LANES], F.at[pl.ds(at, bands), LANES:2 * LANES]

    def difference(L, F, M, load, neighbour):
        for j in range(tiles):
            v = load(j)
            high = v.astype(jnp.bfloat16)
            low = (v - high.astype(jnp.float32)).astype(jnp.bfloat16)
            L[pl.ds(j * pitch_m, bands), 0:LANES] = high
            L[pl.ds(j * pitch_m, bands), LANES:2 * LANES] = low
        F[...] = jnp.dot(L[...], M[...], preferred_element_type=jnp.float32)
        return lambda j: part_of(F, j)[0][...] + part_of(F, j + neighbour)[1][...]

    def right_diff(load):
        return difference(LA, FA, MA, load, 1)

    def left_diff(load):
        return difference(LB, FB, MB, load, -1)

    at_in = lax.broadcasted_iota(jnp.int32, (2 * LANES, 2 * LANES), 0) % LANES
    at_out = lax.broadcasted_iota(jnp.int32, (2 * LANES, 2 * LANES), 1)

    def plus(cond):
        return jnp.where(cond, 1.0, 0.0)
    inside = at_out < LANES
    MA[...] = (plus(inside & (at_in == at_out + 1)) - plus(inside & (at_in == at_out))
               + plus((at_out == 2 * LANES - 1) & (at_in == 0))).astype(jnp.bfloat16)
    MB[...] = (plus(inside & (at_in == at_out)) - plus(inside & (at_in == at_out - 1))
               - plus((at_out == LANES) & (at_in == LANES - 1))).astype(jnp.bfloat16)
    LA[...] = jnp.zeros_like(LA)
    LB[...] = jnp.zeros_like(LB)

    pl.semaphore_wait(barrier, count)

    lane = lax.broadcasted_iota(jnp.int32, (1, wide), 1)
    column = ci * cols + jnp.where(lane < cols + LANES // 2, lane, lane - wide)
    CY[...] = jnp.where((column >= 0) & (column < n_col * cols - 1), STEP, 0.0)

    def put_weight(r, _):
        N[r, pl.ds(bands, 8), 0:cols] = jnp.broadcast_to(w_ref[pl.ds(r, 1), :], (8, cols))
        return 0
    lax.fori_loop(0, rows, put_weight, 0)
    S[:, pl.ds(8, 8), :] = jnp.zeros((ITERS, 8, wide), jnp.float32)

    @pl.when(jnp.logical_not(has_down))
    def _():
        HU[...] = jnp.zeros_like(HU)

    @pl.when(jnp.logical_not(has_up))
    def _():
        HD[...] = jnp.zeros_like(HD)

    @pl.when(jnp.logical_not(has_right))
    def _():
        ER[...] = jnp.zeros_like(ER)

    @pl.when(jnp.logical_not(has_left))
    def _():
        EL[...] = jnp.zeros_like(EL)

    fetch.wait()
    y_start(0, 0)

    pitch = 2 * ITERS
    spot = lax.broadcasted_iota(jnp.int32, (8, LANES), 1)

    def pack(g, _):
        span = pl.ds(pl.multiple_of(g * 8, 8), 8)
        acc = jnp.zeros((8, LANES), jnp.float32)
        for r in range(rows):
            at = r * pitch
            head = pltpu.roll(N[r, span, 0:LANES], at % LANES, 1)
            tail = pltpu.roll(N[r, span, cols - LANES:cols], (at + pitch) % LANES, 1)
            acc = jnp.where((spot >= at) & (spot < at + ITERS), head, acc)
            acc = jnp.where((spot >= at + ITERS) & (spot < at + pitch), tail, acc)
        E[span] = acc
        return 0
    lax.fori_loop(0, groups + 1, pack, 0)

    to_left = pltpu.make_async_remote_copy(
        src_ref=E, dst_ref=ER, send_sem=xs.at[0], recv_sem=xr.at[0],
        device_id={"col": ci - 1}, device_id_type=MESH)
    to_right = pltpu.make_async_remote_copy(
        src_ref=E, dst_ref=EL, send_sem=xs.at[1], recv_sem=xr.at[1],
        device_id={"col": ci + 1}, device_id_type=MESH)

    @pl.when(has_left)
    def _():
        to_left.start()

    @pl.when(has_right)
    def _():
        to_right.start()

    @pl.when(has_right)
    def _():
        to_left.wait_recv()

    @pl.when(has_left)
    def _():
        to_right.wait_recv()

    def unpack(g, _):
        span = pl.ds(pl.multiple_of(g * 8, 8), 8)
        from_right, from_left = ER[span], EL[span]
        for r in range(rows):
            at = r * pitch
            head = pltpu.roll(from_right, (LANES - at) % LANES, 1)
            tail = pltpu.roll(from_left, (LANES - at - pitch) % LANES, 1)
            N[r, span, cols:wide] = jnp.where(spot < LANES // 2, head, tail)
        return 0
    lax.fori_loop(0, groups + 1, unpack, 0)
    y_start(0, 1)

    def put_wt(r, _):
        WT[pl.ds(r, 1)] = N[r, pl.ds(bands, 1), :]
        return 0
    lax.fori_loop(0, rows, put_wt, 0)

    full = pl.ds(0, bands)

    def dual_row(r, own, nxt, cx, first, put):
        grad = right_diff(own)
        sums = []
        for j in range(tiles):
            t = tile(j)
            qx = cx * (nxt(j) - own(j))
            qy = CY[:, t] * grad(j)
            if not first:
                sc = SC[r, 0:1, t]
                qx = sc * QX[r, :, t] + qx
                qy = sc * QY[r, :, t] + qy
            QX[r, :, t] = qx
            QY[r, :, t] = qy
            sums.append(jnp.sum(qx * qx + qy * qy, axis=0, keepdims=True))
        put(jnp.concatenate(sums, axis=1))

    def put_main(k, r):
        def put(v):
            S[k, pl.ds(r, 1)] = v
        return put

    def put_edge(k, i):
        def put(v):
            SE[k, pl.ds(i, 1)] = v
        return put

    cx_last = jnp.where(has_down, STEP, 0.0)
    cx_above = jnp.where(has_up, STEP, 0.0)

    def edges(k, field):
        y_recv(k, 0)
        if k == 0:
            y_recv(0, 1)
            WT[pl.ds(rows, 1)] = HD[0, pl.ds(bands, 1), :]
        dual_row(last, lambda j: field[last, full, tile(j)], lambda j: HU[k, full, tile(j)],
                 cx_last, k == 0, put_edge(k, 0))
        dual_row(rows, lambda j: HD[k, full, tile(j)], lambda j: field[0, full, tile(j)],
                 cx_above, k == 0, put_edge(k, 1))
        z_start(k, 2)

    def scaled_y(r):
        return left_diff(lambda j: SC[r, 0:1, tile(j)] * QY[r, :, tile(j)])

    def primal_tile(r, above, j, first, div_y):
        t = tile(j)
        pu = SC[above, 0:1, t] * QX[above, :, t]
        px = SC[r, 0:1, t] * QX[r, :, t]
        div = (px - pu) + div_y(j)
        given = N[r, full, t]
        if first:
            u = given
            new = given + div
        else:
            u = U[r, :, t]
            new = KEEP * u + (GAIN * given + div)
        U[r, :, t] = new
        return pu, new, u

    def primal_row(r, above, first):
        div_y = scaled_y(r)
        for j in range(tiles):
            _, new, u = primal_tile(r, above, j, first, div_y)
            W[r, :, tile(j)] = 2.0 * new - u

    def start_row(r, _):
        dual_row(r, lambda j: N[r, full, tile(j)], lambda j: N[r + 1, full, tile(j)], STEP, True, put_main(0, r))
        return 0
    lax.fori_loop(0, 8, start_row, 0)
    z_start(0, 0)
    lax.fori_loop(8, last, start_row, 0)
    z_start(0, 1)
    edges(0, N)
    sync(0)

    for k in range(1, ITERS):
        first = k == 1
        if k > 1:
            y_sent(k - 1)
        primal_row(0, rows, first)
        primal_row(last, last - 1, first)
        y_start(k)

        def both(r, _, first=first, k=k):
            div_y = scaled_y(r)
            grad = right_diff(lambda j: W[r - 1, :, tile(j)])
            sums = []
            for j in range(tiles):
                t = tile(j)
                pu, new, u = primal_tile(r, r - 1, j, first, div_y)
                w = 2.0 * new - u
                W[r, :, t] = w
                qx = pu + STEP * (w - W[r - 1, :, t])
                qy = SC[r - 1, 0:1, t] * QY[r - 1, :, t] + CY[:, t] * grad(j)
                QX[r - 1, :, t] = qx
                QY[r - 1, :, t] = qy
                sums.append(jnp.sum(qx * qx + qy * qy, axis=0, keepdims=True))
            S[k, pl.ds(r - 1, 1)] = jnp.concatenate(sums, axis=1)
            return 0
        lax.fori_loop(1, 9, both, 0)
        z_start(k, 0)
        lax.fori_loop(9, last, both, 0)
        dual_row(last - 1, lambda j: W[last - 1, :, tile(j)], lambda j: W[last, :, tile(j)],
                 STEP, False, put_main(k, last - 1))
        z_start(k, 1)
        edges(k, W)
        sync(k)

    def finish(r, above):
        div_y = scaled_y(r)
        for j in range(tiles):
            primal_tile(r, above, j, False, div_y)
        pltpu.make_async_copy(U.at[r, :, 0:cols], out_ref.at[r], out_sem.at[r]).start()

    finish(0, rows)

    def finish_row(r, _):
        finish(r, r - 1)
        return 0
    lax.fori_loop(1, rows, finish_row, 0)

    y_sent(0, 0)
    y_sent(0, 1)
    y_sent(ITERS - 1)

    @pl.when(has_left)
    def _():
        to_left.wait_send()

    @pl.when(has_right)
    def _():
        to_right.wait_send()
    for k in range(ITERS):
        for d in range(1, n_band):
            for part in range(3):
                z_copy(k, d, part).wait_send()

    def drain(r, _):
        pltpu.make_async_copy(U.at[r, :, 0:cols], out_ref.at[r], out_sem.at[r]).wait()
        return 0
    lax.fori_loop(0, rows, drain, 0)


def local(n_row, n_col, n_band, noisy, weight_map):
    bands, rows, cols = noisy.shape
    padded = -(-bands // 8) * 8
    x = jnp.transpose(noisy, (1, 0, 2))
    if padded != bands:
        x = jnp.pad(x, ((0, 0), (0, padded - bands), (0, 0)))
    wide = cols + LANES
    f32, bf16 = jnp.float32, jnp.bfloat16
    depth = wide // LANES * (-(-padded // 16) * 16)
    peers = n_band - 1
    dma = pltpu.SemaphoreType.DMA
    out = pl.pallas_call(
        functools.partial(kernel, n_row, n_col, n_band),
        out_shape=jax.ShapeDtypeStruct((rows, padded, cols), f32),
        in_specs=[pl.BlockSpec(memory_space=pl.ANY), pl.BlockSpec(memory_space=pltpu.VMEM)],
        out_specs=pl.BlockSpec(memory_space=pl.ANY),
        scratch_shapes=[
            pltpu.VMEM((rows, padded + 8, wide), f32),
            pltpu.VMEM((rows, padded, wide), f32),
            pltpu.VMEM((rows, padded, wide), f32),
            pltpu.VMEM((rows + 1, padded, wide), f32),
            pltpu.VMEM((rows + 1, padded, wide), f32),
            pltpu.VMEM((ITERS, padded + 8, wide), f32),
            pltpu.VMEM((ITERS, padded + 8, wide), f32),
            pltpu.VMEM((padded + 8, LANES), f32),
            pltpu.VMEM((padded + 8, LANES), f32),
            pltpu.VMEM((padded + 8, LANES), f32),
            pltpu.VMEM((rows + 8, wide), f32),
            pltpu.VMEM((rows + 1, 8, wide), f32),
            pltpu.VMEM((1, wide), f32),
            pltpu.VMEM((ITERS, rows, wide), f32),
            pltpu.VMEM((ITERS, 2, wide), f32),
            pltpu.VMEM((ITERS, peers, rows, wide), f32),
            pltpu.VMEM((ITERS, peers, 2, wide), f32),
            pltpu.VMEM((depth, 2 * LANES), bf16),
            pltpu.VMEM((depth, 2 * LANES), bf16),
            pltpu.VMEM((depth, 2 * LANES), f32),
            pltpu.VMEM((depth, 2 * LANES), f32),
            pltpu.VMEM((2 * LANES, 2 * LANES), bf16),
            pltpu.VMEM((2 * LANES, 2 * LANES), bf16),
            dma, dma((rows,)),
            dma((2, ITERS + 1)), dma((2, ITERS + 1)),
            dma((2,)), dma((2,)),
            dma((ITERS, peers, 3)), dma((ITERS, peers, 3)),
        ],
        compiler_params=pltpu.CompilerParams(
            collective_id=0, has_side_effects=True, vmem_limit_bytes=48 * 1024 * 1024),
    )(x, weight_map)
    return jnp.transpose(out[:, :bands], (1, 0, 2))


def solution(mesh):
    placed = (P("band", "row", "col"), P("row", "col"))
    sizes = dict(mesh.shape)
    body = functools.partial(local, sizes["row"], sizes["col"], sizes["band"])
    return jax.shard_map(
        body, mesh=mesh, in_specs=placed, out_specs=P("band", "row", "col"), check_vma=False
    )
```

```python
import functools

import jax
import jax.numpy as jnp
from jax import lax
from jax.experimental import pallas as pl
from jax.experimental.pallas import tpu as pltpu
from jax.sharding import PartitionSpec as P

ITERS = 4
dual_step = 0.35
primal_step = 0.35
KEEP = 1.0 / (1.0 + primal_step)
GAIN = primal_step / (1.0 + primal_step)
STEP = GAIN * dual_step
LANES = 128
MESH = pl.DeviceIdType.MESH


def kernel(n_row, n_col, n_band, x_ref, w_ref, out_ref,
           N, U, W, QX, QY, HU, HD, E, ER, EL, WT, SC, CY, S, SE, R, RE,
           LA, LB, FA, FB, MA, MB,
           in_sem, out_sem, ys, yr, xs, xr, zs, zr):
    bands, rows, cols = x_ref.shape
    wide = cols + LANES
    groups = bands // 8
    last = rows - 1
    ri = lax.axis_index("row")
    ci = lax.axis_index("col")
    bi = lax.axis_index("band")
    has_up = ri > 0
    has_down = ri < n_row - 1
    has_left = ci > 0
    has_right = ci < n_col - 1

    fetches = [pltpu.make_async_copy(x_ref.at[:, r, :], N.at[r, 0:bands, 0:cols], in_sem.at[r])
               for r in range(rows)]
    for copy in fetches:
        copy.start()

    barrier = pltpu.get_barrier_semaphore()
    for cond, axis, target in ((has_up, "row", ri - 1), (has_down, "row", ri + 1),
                               (has_left, "col", ci - 1), (has_right, "col", ci + 1)):
        @pl.when(cond)
        def _():
            pl.semaphore_signal(barrier, inc=1, device_id={axis: target}, device_id_type=MESH)
    for d in range(1, n_band):
        pl.semaphore_signal(barrier, inc=1, device_id={"band": lax.rem(bi + d, n_band)}, device_id_type=MESH)
    count = (n_band - 1 + has_up.astype(jnp.int32) + has_down.astype(jnp.int32)
             + has_left.astype(jnp.int32) + has_right.astype(jnp.int32))

    def up_copy(i, src, dst):
        return pltpu.make_async_remote_copy(
            src_ref=src, dst_ref=dst, send_sem=ys.at[0, i], recv_sem=yr.at[0, i],
            device_id={"row": ri - 1}, device_id_type=MESH)

    def down_copy(i, src, dst):
        return pltpu.make_async_remote_copy(
            src_ref=src, dst_ref=dst, send_sem=ys.at[1, i], recv_sem=yr.at[1, i],
            device_id={"row": ri + 1}, device_id_type=MESH)

    def y_pair(k, part):
        if k == 0:
            span = pl.ds(0, cols) if part == 0 else pl.ds(cols, LANES)
            i = 0 if part == 0 else ITERS
            return (up_copy(i, N.at[0, :, span], HU.at[0, :, span]),
                    down_copy(i, N.at[last, :, span], HD.at[0, :, span]))
        span = pl.ds(0, bands)
        return (up_copy(k, W.at[0], HU.at[k, span]), down_copy(k, W.at[last], HD.at[k, span]))

    def y_start(k, part=0):
        up, down = y_pair(k, part)

        @pl.when(has_up)
        def _():
            up.start()

        @pl.when(has_down)
        def _():
            down.start()

    def y_recv(k, part=0):
        up, down = y_pair(k, part)

        @pl.when(has_down)
        def _():
            up.wait_recv()

        @pl.when(has_up)
        def _():
            down.wait_recv()

    def y_sent(k, part=0):
        up, down = y_pair(k, part)

        @pl.when(has_up)
        def _():
            up.wait_send()

        @pl.when(has_down)
        def _():
            down.wait_send()

    def z_copy(k, d, part):
        if part < 2:
            half = pl.ds(part * 8, 8)
            src, dst = S.at[k, half], R.at[k, d - 1, half]
        else:
            src, dst = SE.at[k], RE.at[k, d - 1]
        return pltpu.make_async_remote_copy(
            src_ref=src, dst_ref=dst, send_sem=zs.at[k, d - 1, part], recv_sem=zr.at[k, d - 1, part],
            device_id={"band": lax.rem(bi + d, n_band)}, device_id_type=MESH)

    def z_start(k, part):
        for d in range(1, n_band):
            z_copy(k, d, part).start()

    def total(k, part):
        for d in range(1, n_band):
            z_copy(k, d, part).wait_recv()
        if part < 2:
            half = pl.ds(part * 8, 8)
            acc = S[k, half]
            for d in range(1, n_band):
                acc = acc + R[k, d - 1, half]
            return acc
        acc = SE[k]
        for d in range(1, n_band):
            acc = acc + RE[k, d - 1]
        return acc

    def scale_of(weight, squares):
        return weight / jnp.maximum(weight, jnp.sqrt(1.0 + squares * (1.0 / (GAIN * GAIN))))

    def put_scale(r, v):
        SC[r] = jnp.broadcast_to(v, (8, wide))

    def sync(k):
        for part in range(2):
            half = pl.ds(part * 8, 8)
            values = scale_of(WT[half], total(k, part))
            for i in range(8):
                if part * 8 + i < last:
                    put_scale(part * 8 + i, values[i:i + 1])
        edge = total(k, 2)
        put_scale(last, scale_of(WT[pl.ds(last, 1)], edge[0:1]))
        put_scale(rows, scale_of(WT[pl.ds(rows, 1)], edge[1:2]))

    tiles = wide // LANES
    pitch_m = LA.shape[0] // tiles

    def tile(j):
        return pl.ds((j % tiles) * LANES, LANES)

    def part_of(F, j):
        at = (j % tiles) * pitch_m
        return F.at[pl.ds(at, bands), 0:LANES], F.at[pl.ds(at, bands), LANES:2 * LANES]

    def difference(L, F, M, load, neighbour):
        for j in range(tiles):
            v = load(j)
            high = v.astype(jnp.bfloat16)
            low = (v - high.astype(jnp.float32)).astype(jnp.bfloat16)
            L[pl.ds(j * pitch_m, bands), 0:LANES] = high
            L[pl.ds(j * pitch_m, bands), LANES:2 * LANES] = low
        F[...] = jnp.dot(L[...], M[...], preferred_element_type=jnp.float32)
        return lambda j: part_of(F, j)[0][...] + part_of(F, j + neighbour)[1][...]

    def right_diff(load):
        return difference(LA, FA, MA, load, 1)

    def left_diff(load):
        return difference(LB, FB, MB, load, -1)

    at_in = lax.broadcasted_iota(jnp.int32, (2 * LANES, 2 * LANES), 0) % LANES
    at_out = lax.broadcasted_iota(jnp.int32, (2 * LANES, 2 * LANES), 1)

    def plus(cond):
        return jnp.where(cond, 1.0, 0.0)
    inside = at_out < LANES
    MA[...] = (plus(inside & (at_in == at_out + 1)) - plus(inside & (at_in == at_out))
               + plus((at_out == 2 * LANES - 1) & (at_in == 0))).astype(jnp.bfloat16)
    MB[...] = (plus(inside & (at_in == at_out)) - plus(inside & (at_in == at_out - 1))
               - plus((at_out == LANES) & (at_in == LANES - 1))).astype(jnp.bfloat16)
    LA[...] = jnp.zeros_like(LA)
    LB[...] = jnp.zeros_like(LB)

    pl.semaphore_wait(barrier, count)

    lane = lax.broadcasted_iota(jnp.int32, (1, wide), 1)
    column = ci * cols + jnp.where(lane < cols + LANES // 2, lane, lane - wide)
    CY[...] = jnp.where((column >= 0) & (column < n_col * cols - 1), STEP, 0.0)

    def put_weight(r, _):
        N[r, pl.ds(bands, 8), 0:cols] = jnp.broadcast_to(w_ref[pl.ds(r, 1), :], (8, cols))
        return 0
    lax.fori_loop(0, rows, put_weight, 0)
    S[:, pl.ds(8, 8), :] = jnp.zeros((ITERS, 8, wide), jnp.float32)

    @pl.when(jnp.logical_not(has_down))
    def _():
        HU[...] = jnp.zeros_like(HU)

    @pl.when(jnp.logical_not(has_up))
    def _():
        HD[...] = jnp.zeros_like(HD)

    @pl.when(jnp.logical_not(has_right))
    def _():
        ER[...] = jnp.zeros_like(ER)

    @pl.when(jnp.logical_not(has_left))
    def _():
        EL[...] = jnp.zeros_like(EL)

    for copy in fetches:
        copy.wait()
    y_start(0, 0)

    pitch = 2 * ITERS
    spot = lax.broadcasted_iota(jnp.int32, (8, LANES), 1)

    def pack(g, _):
        span = pl.ds(pl.multiple_of(g * 8, 8), 8)
        acc = jnp.zeros((8, LANES), jnp.float32)
        for r in range(rows):
            at = r * pitch
            head = pltpu.roll(N[r, span, 0:LANES], at % LANES, 1)
            tail = pltpu.roll(N[r, span, cols - LANES:cols], (at + pitch) % LANES, 1)
            acc = jnp.where((spot >= at) & (spot < at + ITERS), head, acc)
            acc = jnp.where((spot >= at + ITERS) & (spot < at + pitch), tail, acc)
        E[span] = acc
        return 0
    lax.fori_loop(0, groups + 1, pack, 0)

    to_left = pltpu.make_async_remote_copy(
        src_ref=E, dst_ref=ER, send_sem=xs.at[0], recv_sem=xr.at[0],
        device_id={"col": ci - 1}, device_id_type=MESH)
    to_right = pltpu.make_async_remote_copy(
        src_ref=E, dst_ref=EL, send_sem=xs.at[1], recv_sem=xr.at[1],
        device_id={"col": ci + 1}, device_id_type=MESH)

    @pl.when(has_left)
    def _():
        to_left.start()

    @pl.when(has_right)
    def _():
        to_right.start()

    @pl.when(has_right)
    def _():
        to_left.wait_recv()

    @pl.when(has_left)
    def _():
        to_right.wait_recv()

    def unpack(g, _):
        span = pl.ds(pl.multiple_of(g * 8, 8), 8)
        from_right, from_left = ER[span], EL[span]
        for r in range(rows):
            at = r * pitch
            head = pltpu.roll(from_right, (LANES - at) % LANES, 1)
            tail = pltpu.roll(from_left, (LANES - at - pitch) % LANES, 1)
            N[r, span, cols:wide] = jnp.where(spot < LANES // 2, head, tail)
        return 0
    lax.fori_loop(0, groups + 1, unpack, 0)
    y_start(0, 1)

    def put_wt(r, _):
        WT[pl.ds(r, 1)] = N[r, pl.ds(bands, 1), :]
        return 0
    lax.fori_loop(0, rows, put_wt, 0)

    full = pl.ds(0, bands)

    def dual_row(r, own, nxt, cx, first, put):
        grad = right_diff(own)
        sums = []
        for j in range(tiles):
            t = tile(j)
            qx = cx * (nxt(j) - own(j))
            qy = CY[:, t] * grad(j)
            if not first:
                sc = SC[r, 0:1, t]
                qx = sc * QX[r, :, t] + qx
                qy = sc * QY[r, :, t] + qy
            QX[r, :, t] = qx
            QY[r, :, t] = qy
            sums.append(jnp.sum(qx * qx + qy * qy, axis=0, keepdims=True))
        put(jnp.concatenate(sums, axis=1))

    def put_main(k, r):
        def put(v):
            S[k, pl.ds(r, 1)] = v
        return put

    def put_edge(k, i):
        def put(v):
            SE[k, pl.ds(i, 1)] = v
        return put

    cx_last = jnp.where(has_down, STEP, 0.0)
    cx_above = jnp.where(has_up, STEP, 0.0)

    def edges(k, field):
        y_recv(k, 0)
        if k == 0:
            y_recv(0, 1)
            WT[pl.ds(rows, 1)] = HD[0, pl.ds(bands, 1), :]
        dual_row(last, lambda j: field[last, full, tile(j)], lambda j: HU[k, full, tile(j)],
                 cx_last, k == 0, put_edge(k, 0))
        dual_row(rows, lambda j: HD[k, full, tile(j)], lambda j: field[0, full, tile(j)],
                 cx_above, k == 0, put_edge(k, 1))
        z_start(k, 2)

    def scaled_y(r):
        return left_diff(lambda j: SC[r, 0:1, tile(j)] * QY[r, :, tile(j)])

    def primal_tile(r, above, j, first, div_y):
        t = tile(j)
        pu = SC[above, 0:1, t] * QX[above, :, t]
        px = SC[r, 0:1, t] * QX[r, :, t]
        div = (px - pu) + div_y(j)
        given = N[r, full, t]
        if first:
            u = given
            new = given + div
        else:
            u = U[r, :, t]
            new = KEEP * u + (GAIN * given + div)
        U[r, :, t] = new
        return pu, new, u

    def primal_row(r, above, first):
        div_y = scaled_y(r)
        for j in range(tiles):
            _, new, u = primal_tile(r, above, j, first, div_y)
            W[r, :, tile(j)] = 2.0 * new - u

    def start_row(r, _):
        dual_row(r, lambda j: N[r, full, tile(j)], lambda j: N[r + 1, full, tile(j)], STEP, True, put_main(0, r))
        return 0
    lax.fori_loop(0, 8, start_row, 0)
    z_start(0, 0)
    lax.fori_loop(8, last, start_row, 0)
    z_start(0, 1)
    edges(0, N)
    sync(0)

    for k in range(1, ITERS):
        first = k == 1
        if k > 1:
            y_sent(k - 1)
        primal_row(0, rows, first)
        primal_row(last, last - 1, first)
        y_start(k)

        def both(r, _, first=first, k=k):
            div_y = scaled_y(r)
            grad = right_diff(lambda j: W[r - 1, :, tile(j)])
            sums = []
            for j in range(tiles):
                t = tile(j)
                pu, new, u = primal_tile(r, r - 1, j, first, div_y)
                w = 2.0 * new - u
                W[r, :, t] = w
                qx = pu + STEP * (w - W[r - 1, :, t])
                qy = SC[r - 1, 0:1, t] * QY[r - 1, :, t] + CY[:, t] * grad(j)
                QX[r - 1, :, t] = qx
                QY[r - 1, :, t] = qy
                sums.append(jnp.sum(qx * qx + qy * qy, axis=0, keepdims=True))
            S[k, pl.ds(r - 1, 1)] = jnp.concatenate(sums, axis=1)
            return 0
        lax.fori_loop(1, 9, both, 0)
        z_start(k, 0)
        lax.fori_loop(9, last, both, 0)
        dual_row(last - 1, lambda j: W[last - 1, :, tile(j)], lambda j: W[last, :, tile(j)],
                 STEP, False, put_main(k, last - 1))
        z_start(k, 1)
        edges(k, W)
        sync(k)

    def finish(r, above):
        div_y = scaled_y(r)
        for j in range(tiles):
            primal_tile(r, above, j, False, div_y)
        pltpu.make_async_copy(U.at[r, :, 0:cols], out_ref.at[r], out_sem.at[r]).start()

    finish(0, rows)

    def finish_row(r, _):
        finish(r, r - 1)
        return 0
    lax.fori_loop(1, rows, finish_row, 0)

    y_sent(0, 0)
    y_sent(0, 1)
    y_sent(ITERS - 1)

    @pl.when(has_left)
    def _():
        to_left.wait_send()

    @pl.when(has_right)
    def _():
        to_right.wait_send()
    for k in range(ITERS):
        for d in range(1, n_band):
            for part in range(3):
                z_copy(k, d, part).wait_send()

    def drain(r, _):
        pltpu.make_async_copy(U.at[r, :, 0:cols], out_ref.at[r], out_sem.at[r]).wait()
        return 0
    lax.fori_loop(0, rows, drain, 0)


def local(n_row, n_col, n_band, noisy, weight_map):
    bands, rows, cols = noisy.shape
    padded = -(-bands // 8) * 8
    x = noisy
    if padded != bands:
        x = jnp.pad(x, ((0, padded - bands), (0, 0), (0, 0)))
    wide = cols + LANES
    f32, bf16 = jnp.float32, jnp.bfloat16
    depth = wide // LANES * (-(-padded // 16) * 16)
    peers = n_band - 1
    dma = pltpu.SemaphoreType.DMA
    out = pl.pallas_call(
        functools.partial(kernel, n_row, n_col, n_band),
        out_shape=jax.ShapeDtypeStruct((rows, padded, cols), f32),
        in_specs=[pl.BlockSpec(memory_space=pl.ANY), pl.BlockSpec(memory_space=pltpu.VMEM)],
        out_specs=pl.BlockSpec(memory_space=pl.ANY),
        scratch_shapes=[
            pltpu.VMEM((rows, padded + 8, wide), f32),
            pltpu.VMEM((rows, padded, wide), f32),
            pltpu.VMEM((rows, padded, wide), f32),
            pltpu.VMEM((rows + 1, padded, wide), f32),
            pltpu.VMEM((rows + 1, padded, wide), f32),
            pltpu.VMEM((ITERS, padded + 8, wide), f32),
            pltpu.VMEM((ITERS, padded + 8, wide), f32),
            pltpu.VMEM((padded + 8, LANES), f32),
            pltpu.VMEM((padded + 8, LANES), f32),
            pltpu.VMEM((padded + 8, LANES), f32),
            pltpu.VMEM((rows + 8, wide), f32),
            pltpu.VMEM((rows + 1, 8, wide), f32),
            pltpu.VMEM((1, wide), f32),
            pltpu.VMEM((ITERS, rows, wide), f32),
            pltpu.VMEM((ITERS, 2, wide), f32),
            pltpu.VMEM((ITERS, peers, rows, wide), f32),
            pltpu.VMEM((ITERS, peers, 2, wide), f32),
            pltpu.VMEM((depth, 2 * LANES), bf16),
            pltpu.VMEM((depth, 2 * LANES), bf16),
            pltpu.VMEM((depth, 2 * LANES), f32),
            pltpu.VMEM((depth, 2 * LANES), f32),
            pltpu.VMEM((2 * LANES, 2 * LANES), bf16),
            pltpu.VMEM((2 * LANES, 2 * LANES), bf16),
            dma((rows,)), dma((rows,)),
            dma((2, ITERS + 1)), dma((2, ITERS + 1)),
            dma((2,)), dma((2,)),
            dma((ITERS, peers, 3)), dma((ITERS, peers, 3)),
        ],
        compiler_params=pltpu.CompilerParams(
            collective_id=0, has_side_effects=True, vmem_limit_bytes=48 * 1024 * 1024),
    )(x, weight_map)
    return jnp.transpose(out[:, :bands], (1, 0, 2))


def solution(mesh):
    placed = (P("band", "row", "col"), P("row", "col"))
    sizes = dict(mesh.shape)
    body = functools.partial(local, sizes["row"], sizes["col"], sizes["band"])
    return jax.shard_map(
        body, mesh=mesh, in_specs=placed, out_specs=P("band", "row", "col"), check_vma=False
    )
```
